256 devices in a mesh: blk: 64 (over y_lo, z, x), mp: 4 (over y_hi, core).
Axes of the slice: x: 4, y: 4 (y_hi: 2, y_lo: 2; y = y_hi * 2 + y_lo), z: 8, core: 2. Of those that a mesh axis runs over, the one named last changes fastest.
Arguments:
- tokens: bfloat16 [64, 320, 7168], P('blk', 'mp'), may hold values from -6 to 6
- cotangent: bfloat16 [64, 320, 7168], P('blk', 'mp'), may hold values from -6 to 6
- gate_weight: bfloat16 [64, 7168, 512], P('blk', None, 'mp'), may hold values from -6 to 6
- up_weight: bfloat16 [64, 7168, 512], P('blk', None, 'mp'), may hold values from -6 to 6
- down_weight: bfloat16 [64, 512, 7168], P('blk', 'mp'), may hold values from -6 to 6
- mass: float32 [64], P('blk'), may hold values from 0.25 to 4
Outputs:
- gate_next: bfloat16 [64, 7168, 512], P('blk', None, 'mp')
- up_next: bfloat16 [64, 7168, 512], P('blk', None, 'mp')
- down_next: bfloat16 [64, 512, 7168], P('blk', 'mp')
- mass_next: float32 [64], P('blk')
- mass_total: float32 [], replicated
The draws below stay inside these ranges and needn't reach their ends.
All inputs are finite; a program needn't handle non-finite values.
Results may differ from the reference program's by a relative error of at most 0.0051.
Values may be sent and summed in bfloat16 or wider, within the bound.
No kernel may reach another device: no remote copies, remote signals or barrier semaphores. Data moves between devices by JAX's collectives and lax.ppermute only.
A program may use at most 128 MiB of HBM per device.

```python
import math
import jax
import jax.numpy as jnp
from jax import lax

D = 7168
TOK = 320
HID = 512
REPLICAS = 64


def level_of(stream_key, extent, cuts, low, top_value):
    level, own = 1.0, jax.random.fold_in(stream_key, 6)
    for axis_at, parts in cuts:
        steps = jnp.exp(jax.random.uniform(jax.random.fold_in(own, axis_at), (parts,), jnp.float32, low / len(cuts), top_value / len(cuts)))
        level = level * jnp.repeat(steps, extent[axis_at] // parts).reshape([-1 if axis == axis_at else 1 for axis in range(len(extent))])
    return level


def gaussian(stream_key, dims, spread, most, pieces=(), kind=jnp.bfloat16):
    result = spread * jax.random.normal(stream_key, dims, jnp.float32)
    if pieces:
        result = result * level_of(stream_key, dims, pieces, -0.22, 0.18)
    return jnp.clip(result, -most, most).astype(kind)


def setup_inputs(seed: int = 0) -> dict:
    splits = jax.random.split(jax.random.key(seed), 7)
    return {
        "tokens": gaussian(splits[0], (REPLICAS, TOK, D), 1.0, 6.0, ((0, 64), (1, 4))),
        "cotangent": gaussian(splits[1], (REPLICAS, TOK, D), 1.0, 6.0, ((0, 64), (1, 4))),
        "gate_weight": gaussian(splits[2], (REPLICAS, D, HID), 1.0, 6.0, ((0, 64), (2, 4))),
        "up_weight": gaussian(splits[3], (REPLICAS, D, HID), 1.0, 6.0, ((0, 64), (2, 4))),
        "down_weight": gaussian(splits[4], (REPLICAS, HID, D), 1.0, 6.0, ((0, 64), (1, 4))),
        "mass": jnp.clip(jnp.exp(math.log(4.0) - 2.7725887 * jax.random.uniform(splits[5], (REPLICAS,), jnp.float32) ** level_of(splits[5], (REPLICAS,), ((0, 64),), -0.2, 0.2)), 0.25, 4.0),
    }


step_size = 0.5


def replica_numerators(x, dy, wg, wu, wd, weight):
    inv_d = D ** -0.5
    inv_h = HID ** -0.5
    gate_pre = jnp.dot(x, wg, preferred_element_type=jnp.float32) * inv_d
    up_pre = jnp.dot(x, wu, preferred_element_type=jnp.float32) * inv_d
    sig = jax.nn.sigmoid(gate_pre)
    hidden = (gate_pre * sig * up_pre).astype(jnp.bfloat16)
    hidden_grad = jnp.dot(dy, wd.T, preferred_element_type=jnp.float32) * inv_h
    gate_gp = (hidden_grad * up_pre * sig * (1.0 + gate_pre * (1.0 - sig))).astype(jnp.bfloat16)
    up_gp = (hidden_grad * gate_pre * sig).astype(jnp.bfloat16)
    gate_grad = jnp.dot(x.T, gate_gp, preferred_element_type=jnp.float32) * inv_d
    up_grad = jnp.dot(x.T, up_gp, preferred_element_type=jnp.float32) * inv_d
    down_grad = jnp.dot(hidden.T, dy, preferred_element_type=jnp.float32) * inv_h
    numer_gate = (weight * (wg.astype(jnp.float32) - step_size * gate_grad)).astype(jnp.bfloat16)
    numer_up = (weight * (wu.astype(jnp.float32) - step_size * up_grad)).astype(jnp.bfloat16)
    numer_down = (weight * (wd.astype(jnp.float32) - step_size * down_grad)).astype(jnp.bfloat16)
    return numer_gate, numer_up, numer_down


def reference(tokens, cotangent, gate_weight, up_weight, down_weight, mass):
    def one(index):
        return replica_numerators(tokens[index], cotangent[index], gate_weight[index],
                                  up_weight[index], down_weight[index], mass[index])

    numer_gate, numer_up, numer_down = lax.map(one, jnp.arange(REPLICAS, dtype=jnp.int32))
    mass_next = (mass + 3.0 * jnp.roll(mass, 1) + 3.0 * jnp.roll(mass, 2) + jnp.roll(mass, 3)) / 8.0

    def mix(index):
        outs = []
        for numer in (numer_gate, numer_up, numer_down):
            first = numer[(index - 1) % REPLICAS].astype(jnp.float32)
            second = numer[(index - 2) % REPLICAS].astype(jnp.float32)
            third = numer[(index - 3) % REPLICAS].astype(jnp.float32)
            total = numer[index].astype(jnp.float32) + 3.0 * first + 3.0 * second + third
            outs.append(((total / 8.0) / mass_next[index]).astype(jnp.bfloat16))
        return tuple(outs)

    gate_next, up_next, down_next = lax.map(mix, jnp.arange(REPLICAS, dtype=jnp.int32))
    mass_total = jnp.sum(mass_next)
    return gate_next, up_next, down_next, mass_next, mass_total
```

```python
import jax
import jax.numpy as jnp
from jax import lax
from jax.sharding import PartitionSpec as P


step_size = 0.5
ROW = 4
DOWN_CUTS = (0, 18, 37, 56)
GATE_CUTS = (0, 19, 38, 56)
UP_CUTS = (0, 19, 38, 56)


def cuts(width, marks):
    return [slice(width * a // 56, width * b // 56) for a, b in zip(marks[:-1], marks[1:])]


def swapped(array, mask):
    count = lax.axis_size("mp")
    return lax.ppermute(array, "mp", [(i, i ^ mask) for i in range(count)])


def moved(array, shift):
    count = lax.axis_size("blk")
    pairs = [(r, (r + shift[r % ROW]) % count) for r in range(count) if shift[r % ROW] is not None]
    return lax.ppermute(array, "blk", pairs)


def everyone(value):
    count = lax.axis_size("blk")
    ring = jnp.where(lax.iota(jnp.int32, count) == lax.axis_index("blk"), value, 0.0)
    bits = [1 << k for k in range(count.bit_length() - 1)]
    for bit in bits:
        other = lax.ppermute(ring, "blk", [(r, r ^ bit) for r in range(count)])
        ring = ring + other
    return ring


def mixed(numer, place, scale):
    f32 = jnp.float32
    even = place % 2 == 0
    above = moved(numer, (None, 4, 4, 4))
    crossing = jnp.where(place < 2, numer, above)
    got = moved(crossing, (3, 1, -1, -3))
    part = jnp.where(even, 3.0 * numer.astype(f32), above.astype(f32)) + 3.0 * got.astype(f32)
    part = part.astype(jnp.bfloat16)
    partner = moved(part, (1, -1, 1, -1))
    total = numer.astype(f32) + jnp.where(even, 3.0, 1.0) * got.astype(f32)
    return ((total + partner.astype(f32)) * scale).astype(jnp.bfloat16)


def on_device(tokens, cotangent, gate_weight, up_weight, down_weight, mass):
    f32 = jnp.float32
    bf16 = jnp.bfloat16
    x0 = tokens[0]
    d0 = cotangent[0]
    gate_w = gate_weight[0]
    up_w = up_weight[0]
    down_w = down_weight[0]
    width = gate_w.shape[0]
    units = gate_w.shape[1]
    inv_d = width ** (-0.5)
    inv_h = (units * lax.axis_size("mp")) ** (-0.5)
    spans = cuts(width, DOWN_CUTS)
    gate_spans = cuts(width, GATE_CUTS)
    up_spans = cuts(width, UP_CUTS)

    x2 = swapped(x0, 2)
    x1 = swapped(x0, 1)
    d2 = [swapped(d0[:, s], 2) for s in spans]
    d1 = swapped(d0, 1)
    x3 = swapped(x2, 1)
    d3 = [swapped(d, 1) for d in d2]

    me = lax.axis_index("blk")
    masses = everyone(mass)
    next_all = (
        masses + 3.0 * jnp.roll(masses, 1) + 3.0 * jnp.roll(masses, 2) + jnp.roll(masses, 3)
    ) / 8.0
    mass_total = jnp.sum(next_all)
    mass_next = lax.dynamic_slice(next_all, (me,), (1,))
    place = me % ROW
    scale = 0.125 / mass_next[0]

    x = jnp.concatenate([x0, x1, x2, x3], axis=0)
    gate_pre = jnp.dot(x, gate_w, preferred_element_type=f32) * inv_d
    up_pre = jnp.dot(x, up_w, preferred_element_type=f32) * inv_d
    sig = jax.nn.sigmoid(gate_pre)
    hidden = (gate_pre * sig * up_pre).astype(bf16)

    dy = [jnp.concatenate([d0[:, s], d1[:, s], d2[c], d3[c]], axis=0) for c, s in enumerate(spans)]
    weight = mass[0]
    rows = (((0,), (0,)), ((), ()))

    def numer(w, lhs, rhs, scale_by):
        grad = lax.dot_general(lhs, rhs, rows, preferred_element_type=f32) * scale_by
        return (weight * (w.astype(f32) - step_size * grad)).astype(bf16)

    down_numer = [numer(down_w[:, s], hidden, dy[c], inv_h) for c, s in enumerate(spans)]
    down_next = [mixed(n, place, scale) for n in down_numer]
    gate_pre, up_pre, _ = lax.optimization_barrier((gate_pre, up_pre, down_numer[-1]))
    sig = jax.nn.sigmoid(gate_pre)
    hidden_grad = 0.0
    for c, s in enumerate(spans):
        hidden_grad = hidden_grad + lax.dot_general(
            dy[c], down_w[:, s], (((1,), (1,)), ((), ())), preferred_element_type=f32
        )
    hidden_grad = hidden_grad * inv_h
    gate_gp = (hidden_grad * up_pre * sig * (1.0 + gate_pre * (1.0 - sig))).astype(bf16)
    up_gp = (hidden_grad * gate_pre * sig).astype(bf16)
    gate_next = [mixed(numer(gate_w[s], x[:, s], gate_gp, inv_d), place, scale) for s in gate_spans]
    up_next = [mixed(numer(up_w[s], x[:, s], up_gp, inv_d), place, scale) for s in up_spans]
    return (
        jnp.concatenate(gate_next, axis=0)[None],
        jnp.concatenate(up_next, axis=0)[None],
        jnp.concatenate(down_next, axis=1)[None],
        mass_next,
        mass_total,
    )


def solution(mesh):
    in_specs = (
        P("blk", "mp", None),
        P("blk", "mp", None),
        P("blk", None, "mp"),
        P("blk", None, "mp"),
        P("blk", "mp", None),
        P("blk"),
    )
    out_specs = (P("blk", None, "mp"), P("blk", None, "mp"), P("blk", "mp", None), P("blk"), P())

    return jax.shard_map(
        on_device, mesh=mesh, in_specs=in_specs, out_specs=out_specs, check_vma=False
    )
```

```python
import jax
import jax.numpy as jnp
from jax import lax
from jax.sharding import PartitionSpec as P


step_size = 0.5
ROW = 4
DOWN_CUTS = (0, 18, 37, 56)
GATHER_CUTS = (0, 37, 56)
GATE_CUTS = (0, 19, 38, 56)
UP_CUTS = (0, 19, 38, 56)


def cuts(width, marks):
    return [slice(width * a // 56, width * b // 56) for a, b in zip(marks[:-1], marks[1:])]


def swapped(array, mask):
    count = lax.axis_size("mp")
    return lax.ppermute(array, "mp", [(i, i ^ mask) for i in range(count)])


def moved(array, shift):
    count = lax.axis_size("blk")
    pairs = [(r, (r + shift[r % ROW]) % count) for r in range(count) if shift[r % ROW] is not None]
    return lax.ppermute(array, "blk", pairs)


def everyone(value):
    count = lax.axis_size("blk")
    ring = jnp.where(lax.iota(jnp.int32, count) == lax.axis_index("blk"), value, 0.0)
    bits = [1 << k for k in range(count.bit_length() - 1)]
    for bit in bits:
        other = lax.ppermute(ring, "blk", [(r, r ^ bit) for r in range(count)])
        ring = ring + other
    return ring


def mixed(numer, place, scale):
    f32 = jnp.float32
    even = place % 2 == 0
    above = moved(numer, (None, 4, 4, 4))
    crossing = jnp.where(place < 2, numer, above)
    got = moved(crossing, (3, 1, -1, -3))
    part = jnp.where(even, 3.0 * numer.astype(f32), above.astype(f32)) + 3.0 * got.astype(f32)
    part = part.astype(jnp.bfloat16)
    partner = moved(part, (1, -1, 1, -1))
    total = numer.astype(f32) + jnp.where(even, 3.0, 1.0) * got.astype(f32)
    return ((total + partner.astype(f32)) * scale).astype(jnp.bfloat16)


def on_device(tokens, cotangent, gate_weight, up_weight, down_weight, mass):
    f32 = jnp.float32
    bf16 = jnp.bfloat16
    x0 = tokens[0]
    d0 = cotangent[0]
    gate_w = gate_weight[0]
    up_w = up_weight[0]
    down_w = down_weight[0]
    width = gate_w.shape[0]
    units = gate_w.shape[1]
    inv_d = width ** (-0.5)
    inv_h = (units * lax.axis_size("mp")) ** (-0.5)
    spans = cuts(width, DOWN_CUTS)
    gate_spans = cuts(width, GATE_CUTS)
    up_spans = cuts(width, UP_CUTS)

    x2 = swapped(x0, 2)
    x1 = swapped(x0, 1)
    halves = cuts(width, GATHER_CUTS)
    d2 = [swapped(d0[:, s], 2) for s in halves]
    d1 = swapped(d0, 1)
    x3 = swapped(x2, 1)
    d3 = [swapped(d, 1) for d in d2]

    me = lax.axis_index("blk")
    masses = everyone(mass)
    next_all = (
        masses + 3.0 * jnp.roll(masses, 1) + 3.0 * jnp.roll(masses, 2) + jnp.roll(masses, 3)
    ) / 8.0
    mass_total = jnp.sum(next_all)
    mass_next = lax.dynamic_slice(next_all, (me,), (1,))
    place = me % ROW
    scale = 0.125 / mass_next[0]

    x = jnp.concatenate([x0, x1, x2, x3], axis=0)
    both = jnp.concatenate([gate_w, up_w], axis=1)
    pre = jnp.dot(x, both, preferred_element_type=f32) * inv_d
    gate_pre = pre[:, :units]
    up_pre = pre[:, units:]
    sig = jax.nn.sigmoid(gate_pre)
    hidden = (gate_pre * sig * up_pre).astype(bf16)

    dy = [jnp.concatenate([d0[:, s], d1[:, s], d2[c], d3[c]], axis=0) for c, s in enumerate(halves)]
    dy_spans = [dy[0][:, spans[0]], dy[0][:, spans[1]], dy[1]]
    weight = mass[0]
    rows = (((0,), (0,)), ((), ()))

    def numer(w, lhs, rhs, scale_by):
        grad = lax.dot_general(lhs, rhs, rows, preferred_element_type=f32) * scale_by
        return (weight * (w.astype(f32) - step_size * grad)).astype(bf16)

    down_numer = [numer(down_w[:, s], hidden, dy_spans[c], inv_h) for c, s in enumerate(spans)]
    down_next = [mixed(n, place, scale) for n in down_numer]
    gate_pre, up_pre, _ = lax.optimization_barrier((gate_pre, up_pre, down_numer[-1]))
    sig = jax.nn.sigmoid(gate_pre)
    hidden_grad = 0.0
    for c, s in enumerate(halves):
        hidden_grad = hidden_grad + lax.dot_general(
            dy[c], down_w[:, s], (((1,), (1,)), ((), ())), preferred_element_type=f32
        )
    hidden_grad = hidden_grad * inv_h
    gate_gp = (hidden_grad * up_pre * sig * (1.0 + gate_pre * (1.0 - sig))).astype(bf16)
    up_gp = (hidden_grad * gate_pre * sig).astype(bf16)
    gate_next = [mixed(numer(gate_w[s], x[:, s], gate_gp, inv_d), place, scale) for s in gate_spans]
    up_next = [mixed(numer(up_w[s], x[:, s], up_gp, inv_d), place, scale) for s in up_spans]
    return (
        jnp.concatenate(gate_next, axis=0)[None],
        jnp.concatenate(up_next, axis=0)[None],
        jnp.concatenate(down_next, axis=1)[None],
        mass_next,
        mass_total,
    )


def solution(mesh):
    in_specs = (
        P("blk", "mp", None),
        P("blk", "mp", None),
        P("blk", None, "mp"),
        P("blk", None, "mp"),
        P("blk", "mp", None),
        P("blk"),
    )
    out_specs = (P("blk", None, "mp"), P("blk", None, "mp"), P("blk", "mp", None), P("blk"), P())

    return jax.shard_map(
        on_device, mesh=mesh, in_specs=in_specs, out_specs=out_specs, check_vma=False
    )
```

```python
import jax
import jax.numpy as jnp
from jax import lax
from jax.sharding import PartitionSpec as P


step_size = 0.5
PIECES = 3
ROW = 4
DOWN_CUTS = (0, 18, 37, 56)
GATHER_CUTS = (0, 37, 56)
GATE_CUTS = (0, 19, 38, 56)
UP_CUTS = (0, 19, 38, 56)


def cuts(width, marks):
    return [slice(width * a // 56, width * b // 56) for a, b in zip(marks[:-1], marks[1:])]


def swapped(array, mask):
    count = lax.axis_size("mp")
    return lax.ppermute(array, "mp", [(i, i ^ mask) for i in range(count)])


def moved(array, shift):
    count = lax.axis_size("blk")
    pairs = [(r, (r + shift[r % ROW]) % count) for r in range(count) if shift[r % ROW] is not None]
    return lax.ppermute(array, "blk", pairs)


def everyone(value):
    count = lax.axis_size("blk")
    ring = jnp.where(lax.iota(jnp.int32, count) == lax.axis_index("blk"), value, 0.0)
    bits = [1 << k for k in range(count.bit_length() - 1)]
    for bit in bits:
        other = lax.ppermute(ring, "blk", [(r, r ^ bit) for r in range(count)])
        ring = ring + other
    return ring


def mixed(t, numer, place, scale):
    f32 = jnp.float32
    even = place % 2 == 0
    above = moved(numer, (4, 4, 4, 4) if t == 0 else (None, 4, 4, 4))
    crossing = jnp.where(place < 2, numer, above)
    got = moved(crossing, (3, 1, -1, -3))
    part = jnp.where(even, 3.0 * numer.astype(f32), above.astype(f32)) + 3.0 * got.astype(f32)
    part = part.astype(jnp.bfloat16)
    partner = moved(part, (1, -1, 1, -1))
    total = numer.astype(f32) + jnp.where(even, 3.0, 1.0) * got.astype(f32)
    return ((total + partner.astype(f32)) * scale).astype(jnp.bfloat16)


def on_device(tokens, cotangent, gate_weight, up_weight, down_weight, mass):
    f32 = jnp.float32
    bf16 = jnp.bfloat16
    x0 = tokens[0]
    d0 = cotangent[0]
    gate_w = gate_weight[0]
    up_w = up_weight[0]
    down_w = down_weight[0]
    width = gate_w.shape[0]
    units = gate_w.shape[1]
    inv_d = width ** (-0.5)
    inv_h = (units * lax.axis_size("mp")) ** (-0.5)
    spans = cuts(width, DOWN_CUTS)
    gate_spans = cuts(width, GATE_CUTS)
    up_spans = cuts(width, UP_CUTS)

    x2 = swapped(x0, 2)
    x1, d1 = jnp.split(swapped(jnp.concatenate([x0, d0], axis=0), 1), 2)
    halves = cuts(width, GATHER_CUTS)
    d2 = [swapped(d0[:, s], 2) for s in halves]
    x3 = swapped(x2, 1)
    d3 = [swapped(d, 1) for d in d2]

    me = lax.axis_index("blk")
    masses = everyone(mass)
    next_all = (
        masses + 3.0 * jnp.roll(masses, 1) + 3.0 * jnp.roll(masses, 2) + jnp.roll(masses, 3)
    ) / 8.0
    mass_total = jnp.sum(next_all)
    mass_next = lax.dynamic_slice(next_all, (me,), (1,))
    place = me % ROW
    scale = 0.125 / mass_next[0]

    x = jnp.concatenate([x0, x1, x2, x3], axis=0)
    both = jnp.concatenate([gate_w, up_w], axis=1)
    pre = jnp.dot(x, both, preferred_element_type=f32) * inv_d
    gate_pre = pre[:, :units]
    up_pre = pre[:, units:]
    sig = jax.nn.sigmoid(gate_pre)
    hidden = (gate_pre * sig * up_pre).astype(bf16)

    dy = [jnp.concatenate([d0[:, s], d1[:, s], d2[c], d3[c]], axis=0) for c, s in enumerate(halves)]
    dy_spans = [dy[0][:, spans[0]], dy[0][:, spans[1]], dy[1]]
    weight = mass[0]
    rows = (((0,), (0,)), ((), ()))

    def numer(w, lhs, rhs, scale_by):
        grad = lax.dot_general(lhs, rhs, rows, preferred_element_type=f32) * scale_by
        return (weight * (w.astype(f32) - step_size * grad)).astype(bf16)

    down_numer = [numer(down_w[:, s], hidden, dy_spans[c], inv_h) for c, s in enumerate(spans)]
    down_next = [mixed(c, n, place, scale) for c, n in enumerate(down_numer)]
    gate_pre, up_pre, _ = lax.optimization_barrier((gate_pre, up_pre, down_numer[-1]))
    sig = jax.nn.sigmoid(gate_pre)
    hidden_grad = 0.0
    for c, s in enumerate(halves):
        hidden_grad = hidden_grad + lax.dot_general(
            dy[c], down_w[:, s], (((1,), (1,)), ((), ())), preferred_element_type=f32
        )
    hidden_grad = hidden_grad * inv_h
    gate_gp = (hidden_grad * up_pre * sig * (1.0 + gate_pre * (1.0 - sig))).astype(bf16)
    up_gp = (hidden_grad * gate_pre * sig).astype(bf16)
    gate_next = [
        mixed(PIECES + c, numer(gate_w[s], x[:, s], gate_gp, inv_d), place, scale)
        for c, s in enumerate(gate_spans)
    ]
    up_next = [
        mixed(2 * PIECES + c, numer(up_w[s], x[:, s], up_gp, inv_d), place, scale)
        for c, s in enumerate(up_spans)
    ]
    return (
        jnp.concatenate(gate_next, axis=0)[None],
        jnp.concatenate(up_next, axis=0)[None],
        jnp.concatenate(down_next, axis=1)[None],
        mass_next,
        mass_total,
    )


def solution(mesh):
    in_specs = (
        P("blk", "mp", None),
        P("blk", "mp", None),
        P("blk", None, "mp"),
        P("blk", None, "mp"),
        P("blk", "mp", None),
        P("blk"),
    )
    out_specs = (P("blk", None, "mp"), P("blk", None, "mp"), P("blk", "mp", None), P("blk"), P())

    return jax.shard_map(
        on_device, mesh=mesh, in_specs=in_specs, out_specs=out_specs, check_vma=False
    )
```

```python
import jax
import jax.numpy as jnp
from jax import lax
from jax.sharding import PartitionSpec as P


step_size = 0.5
PIECES = 3
ROW = 4
DOWN_CUTS = (0, 18, 37, 56)
GATHER_CUTS = (0, 28, 56)
GATE_CUTS = (0, 19, 38, 56)
UP_CUTS = (0, 19, 38, 56)


def cuts(width, marks):
    return [slice(width * a // 56, width * b // 56) for a, b in zip(marks[:-1], marks[1:])]


def swapped(array, mask):
    count = lax.axis_size("mp")
    return lax.ppermute(array, "mp", [(i, i ^ mask) for i in range(count)])


def moved(array, shift):
    count = lax.axis_size("blk")
    pairs = [(r, (r + shift[r % ROW]) % count) for r in range(count) if shift[r % ROW] is not None]
    return lax.ppermute(array, "blk", pairs)


def everyone(value):
    count = lax.axis_size("blk")
    ring = jnp.where(lax.iota(jnp.int32, count) == lax.axis_index("blk"), value, 0.0)
    bits = [1 << k for k in range(count.bit_length() - 1)]
    for bit in bits:
        other = lax.ppermute(ring, "blk", [(r, r ^ bit) for r in range(count)])
        ring = ring + other
    return ring


def mixed(t, numer, place, scale):
    f32 = jnp.float32
    even = place % 2 == 0
    above = moved(numer, (4, 4, 4, 4) if t == 0 else (None, 4, 4, 4))
    crossing = jnp.where(place < 2, numer, above)
    got = moved(crossing, (3, 1, -1, -3))
    part = jnp.where(even, 3.0 * numer.astype(f32), above.astype(f32)) + 3.0 * got.astype(f32)
    part = part.astype(jnp.bfloat16)
    partner = moved(part, (1, -1, 1, -1))
    total = numer.astype(f32) + jnp.where(even, 3.0, 1.0) * got.astype(f32)
    return ((total + partner.astype(f32)) * scale).astype(jnp.bfloat16)


def on_device(tokens, cotangent, gate_weight, up_weight, down_weight, mass):
    f32 = jnp.float32
    bf16 = jnp.bfloat16
    x0 = tokens[0]
    d0 = cotangent[0]
    gate_w = gate_weight[0]
    up_w = up_weight[0]
    down_w = down_weight[0]
    width = gate_w.shape[0]
    units = gate_w.shape[1]
    inv_d = width ** (-0.5)
    inv_h = (units * lax.axis_size("mp")) ** (-0.5)
    spans = cuts(width, DOWN_CUTS)
    gate_spans = cuts(width, GATE_CUTS)
    up_spans = cuts(width, UP_CUTS)

    x2 = swapped(x0, 2)
    x1, d1 = jnp.split(swapped(jnp.concatenate([x0, d0], axis=0), 1), 2)
    halves = cuts(width, GATHER_CUTS)
    d2 = [swapped(d0[:, s], 2) for s in halves]
    x3 = swapped(x2, 1)
    d3 = [swapped(d, 1) for d in d2]

    me = lax.axis_index("blk")
    masses = everyone(mass)
    next_all = (
        masses + 3.0 * jnp.roll(masses, 1) + 3.0 * jnp.roll(masses, 2) + jnp.roll(masses, 3)
    ) / 8.0
    mass_total = jnp.sum(next_all)
    mass_next = lax.dynamic_slice(next_all, (me,), (1,))
    place = me % ROW
    scale = 0.125 / mass_next[0]

    x = jnp.concatenate([x0, x1, x2, x3], axis=0)
    both = jnp.concatenate([gate_w, up_w], axis=1)
    pre = jnp.dot(x, both, preferred_element_type=f32) * inv_d
    gate_pre = pre[:, :units]
    up_pre = pre[:, units:]
    sig = jax.nn.sigmoid(gate_pre)
    hidden = (gate_pre * sig * up_pre).astype(bf16)

    dy = [jnp.concatenate([d0[:, s], d1[:, s], d2[c], d3[c]], axis=0) for c, s in enumerate(halves)]
    split = halves[0].stop
    across = [dy[0][:, spans[1].start : split], dy[1][:, : spans[1].stop - split]]
    dy_spans = [
        dy[0][:, spans[0]],
        jnp.concatenate(across, axis=1),
        dy[1][:, spans[2].start - split :],
    ]
    weight = mass[0]
    rows = (((0,), (0,)), ((), ()))

    def numer(w, lhs, rhs, scale_by):
        grad = lax.dot_general(lhs, rhs, rows, preferred_element_type=f32) * scale_by
        return (weight * (w.astype(f32) - step_size * grad)).astype(bf16)

    down_numer = [numer(down_w[:, s], hidden, dy_spans[c], inv_h) for c, s in enumerate(spans)]
    down_next = [mixed(c, n, place, scale) for c, n in enumerate(down_numer)]
    gate_pre, up_pre, _ = lax.optimization_barrier((gate_pre, up_pre, down_numer[-1]))
    sig = jax.nn.sigmoid(gate_pre)
    hidden_grad = 0.0
    for c, s in enumerate(halves):
        hidden_grad = hidden_grad + lax.dot_general(
            dy[c], down_w[:, s], (((1,), (1,)), ((), ())), preferred_element_type=f32
        )
    hidden_grad = hidden_grad * inv_h
    gate_gp = (hidden_grad * up_pre * sig * (1.0 + gate_pre * (1.0 - sig))).astype(bf16)
    up_gp = (hidden_grad * gate_pre * sig).astype(bf16)
    gate_next = [
        mixed(PIECES + c, numer(gate_w[s], x[:, s], gate_gp, inv_d), place, scale)
        for c, s in enumerate(gate_spans)
    ]
    up_next = [
        mixed(2 * PIECES + c, numer(up_w[s], x[:, s], up_gp, inv_d), place, scale)
        for c, s in enumerate(up_spans)
    ]
    return (
        jnp.concatenate(gate_next, axis=0)[None],
        jnp.concatenate(up_next, axis=0)[None],
        jnp.concatenate(down_next, axis=1)[None],
        mass_next,
        mass_total,
    )


def solution(mesh):
    in_specs = (
        P("blk", "mp", None),
        P("blk", "mp", None),
        P("blk", None, "mp"),
        P("blk", None, "mp"),
        P("blk", "mp", None),
        P("blk"),
    )
    out_specs = (P("blk", None, "mp"), P("blk", None, "mp"), P("blk", "mp", None), P("blk"), P())

    return jax.shard_map(
        on_device, mesh=mesh, in_specs=in_specs, out_specs=out_specs, check_vma=False
    )
```
